512 devices in a mesh: bank: 4 (over z_hi), lane: 16 (over y, core), site: 8 (over z_lo, x).
Axes of the slice: x: 4, y: 8, z: 8 (z_hi: 4, z_lo: 2; z = z_hi * 2 + z_lo), core: 2. Of those that a mesh axis runs over, the one named last changes fastest.
Arguments:
- wave_parts: float32 [16, 256, 128, 128], P('site', ('bank', 'lane')), parts along dimension 0, may hold values from -6 to 6
- level_table: float32 [2048, 128, 128], P(('site', 'bank', 'lane')), parts along dimension 0, may hold values from -2 to 2
- phase_angles: float32 [16, 128], P('site'), parts along dimension 0, may hold values from 0.3 to 1.2
- mix_angles: float32 [16, 4], P('site'), parts along dimension 0, may hold values from 0.3 to 1.2
Outputs:
- final_parts: float32 [16, 256, 128, 128], P('site', ('bank', 'lane')), parts along dimension 0
The draws below stay inside these ranges and needn't reach their ends.
There are 8 independent parts, one for each index of `site`. The reference program is written for one: setup_inputs(seed, part) draws one part's arguments, and reference() takes and returns one part's arrays. A program takes and returns all parts, laid end to end along the dimension named above; each array names one. Nothing has to cross between parts.
All inputs are finite; a program needn't handle non-finite values.
Results may differ from the reference program's by a relative error of at most 0.0003.
Values sent between devices are 32-bit elements; how exact they have to be, the bound alone decides.
No kernel may reach another device: no remote copies, remote signals or barrier semaphores. Data moves between devices by JAX's collectives and lax.ppermute only.
A program may use at most 64 MiB of HBM per device.

```python
import jax
import jax.numpy as jnp
from jax import lax

BLOCKS_DEV = 4
ROWS = 128
LANES = 128
BLOCKS = 256
LAYERS = 2
N_BANK = 4
N_LANE = 16


def level_of(key, extent, pieces, low, largest):
    gain, own = 1.0, jax.random.fold_in(key, 6)
    for axis_at, shards_of in pieces:
        heights = jnp.exp(jax.random.uniform(jax.random.fold_in(own, axis_at), (shards_of,), jnp.float32, low / len(pieces), largest / len(pieces)))
        gain = gain * jnp.repeat(heights, extent[axis_at] // shards_of).reshape([-1 if axis == axis_at else 1 for axis in range(len(extent))])
    return gain


def noise(stream_key, dims, deviation, reach, pieces=(), kind=jnp.bfloat16):
    array = jax.random.normal(stream_key, dims, jnp.float32) * deviation
    if len(pieces) > 0:
        array = level_of(stream_key, dims, pieces, -0.22, 0.18) * array
    return jnp.clip(array, min=-reach, max=reach).astype(kind)


def setup_inputs(seed: int = 0, part: int = 0) -> dict:
    arg_keys = jax.random.split(jax.random.key(seed), 5)
    own_keys = jax.random.split(jax.random.fold_in(arg_keys[4], part), 5)
    wave_parts = noise(own_keys[0], (2, BLOCKS, ROWS, LANES), 1.0, 6.0, ((1, 64),), jnp.float32)
    level_table = jnp.clip(jax.random.uniform(own_keys[1], (BLOCKS, ROWS, LANES), jnp.float32, -2.0, 2.0) * level_of(own_keys[1], (BLOCKS, ROWS, LANES), ((0, 64),), -0.4, 0.0), -2.0, 2.0)
    phase_angles = jnp.clip(jax.random.uniform(own_keys[2], (LAYERS, LANES), jnp.float32, 0.3, 1.2), 0.3, 1.2)
    mix_angles = jnp.clip(jax.random.uniform(own_keys[3], (LAYERS, 4), jnp.float32, 0.3, 1.2), 0.3, 1.2)
    return dict(wave_parts=wave_parts, level_table=level_table, phase_angles=phase_angles, mix_angles=mix_angles)


def count_bits(values, count):
    places = jnp.arange(count.bit_length() - 1, dtype=jnp.int32)
    return jnp.sum((values[..., None] >> places) & 1, axis=-1)


def plane_table(count, angle):
    rank = jnp.arange(count, dtype=jnp.int32)
    apart = count_bits(rank[:, None] ^ rank[None, :], count)
    minus = count_bits(rank[:, None] & (rank[:, None] ^ rank[None, :]), count)
    bits = count.bit_length() - 1
    size = jnp.cos(angle) ** (bits - apart).astype(jnp.float32) * jnp.sin(angle) ** apart.astype(jnp.float32)
    return size * jnp.where(minus % 2 == 1, -1.0, 1.0).astype(jnp.float32)


def apply_along(values, dim, angle):
    real_part = plane_table(values.shape[dim], angle)
    def times(table):
        moved = jnp.tensordot(values, table, axes=([dim], [0]), precision=lax.Precision.HIGHEST)
        return jnp.moveaxis(moved, -1, dim)
    return times(real_part)


def turn_phase(values, levels, angle):
    turn = angle * levels
    return jnp.stack([values[0] * jnp.cos(turn) + values[1] * jnp.sin(turn), values[1] * jnp.cos(turn) - values[0] * jnp.sin(turn)])


def reference(wave_parts, level_table, phase_angles, mix_angles):
    values = wave_parts
    for layer in range(LAYERS):
        values = turn_phase(values, level_table, phase_angles[layer])
        values = apply_along(values, 3, mix_angles[layer, 0])
        values = apply_along(values, 2, mix_angles[layer, 1])
        parts = values.reshape(2, N_BANK, N_LANE, BLOCKS_DEV, ROWS, LANES)
        parts = apply_along(parts, 1, mix_angles[layer, 2])
        parts = apply_along(parts, 2, mix_angles[layer, 3])
        parts = apply_along(parts, 3, mix_angles[layer, 2])
        values = parts.reshape(values.shape)
    return values
```

```python
import jax
import jax.numpy as jnp
from jax import lax
from jax.experimental import pallas as pl
from jax.experimental.pallas import tpu as pltpu
from jax.sharding import PartitionSpec as P

SUB = 8
F32 = jnp.float32

SIN = (0.9999999814442071, -0.16666657755521955, 0.008333210982283118, -0.00019834058585468524,
       2.734996203799263e-06, -2.21633008243829e-08)
COS = (0.9999999997000049, -0.4999999949621528, 0.04166665285119409, -0.0013888746708823352,
       2.4794608537121183e-05, -2.7380880775339007e-07, 1.8645524434398867e-09)


def series(z, terms):
    total = z * terms[-1] + terms[-2]
    for term in terms[-3::-1]:
        total = total * z + term
    return total


def cos_sin(x):
    z = x * x
    return series(z, COS), series(z, SIN) * x


def plane_table(cos, sin, left):
    row = lax.broadcasted_iota(jnp.int32, (128, 128), 0)
    col = lax.broadcasted_iota(jnp.int32, (128, 128), 1)
    if left:
        sin = -sin
    table = None
    for bit in range(7):
        at_row, at_col = (row >> bit) & 1, (col >> bit) & 1
        factor = jnp.where(at_row == at_col, cos, jnp.where(at_row == 1, -sin, sin))
        table = factor if table is None else table * factor
    return table


def mix(parts, tan):
    parts = list(parts)
    step = 1
    while step < len(parts):
        for i in range(len(parts)):
            if not i & step:
                u, v = parts[i], parts[i + step]
                parts[i], parts[i + step] = u - tan * v, v + tan * u
        step *= 2
    return parts


def dot(a, b):
    return lax.dot_general(
        a, b, (((1,), (0,)), ((), ())), precision=lax.Precision.HIGHEST, preferred_element_type=F32
    )


def spread(value, shape=(SUB, 128)):
    return jnp.full(shape, value, F32)


def within(parts, lane_table, row_table, tan):
    out = []
    for blocks in parts:
        done = [dot(row_table, dot(block, lane_table)) for block in blocks]
        out.append(mix(done, tan))
    return out


def tables(mix_ref, layer):
    cos0, sin0 = cos_sin(spread(mix_ref[layer, 0], (128, 128)))
    cos1, sin1 = cos_sin(spread(mix_ref[layer, 1], (128, 128)))
    cos2, sin2 = cos_sin(spread(mix_ref[layer, 2], (128, 128)))
    lane_table = plane_table(cos0, sin0, False)
    row_table = plane_table(cos1, sin1, True) * (cos2 * cos2)
    return lane_table, row_table, sin2 / cos2


def first_kernel(mix_ref, wave_ref, level_ref, phase_ref, out_ref):
    lane_table, row_table, tan = tables(mix_ref, 0)
    angle = phase_ref[0:1, :]
    re, im = [], []
    for b in range(4):
        level = level_ref[b]
        cos, sin = cos_sin(level * angle)
        u, v = wave_ref[0, b], wave_ref[1, b]
        re.append(u * cos + v * sin)
        im.append(v * cos - u * sin)
        out_ref[b * 16 : b * 16 + 16, 2] = level.reshape(16, SUB, 128)
    for part, blocks in enumerate(within((re, im), lane_table, row_table, tan)):
        for b in range(4):
            out_ref[b * 16 : b * 16 + 16, part] = blocks[b].reshape(16, SUB, 128)


def middle_kernel(mix_ref, phase_ref, in_ref, out_ref, work_ref):
    scale, tans = None, []
    for layer in range(2):
        cos2, sin2 = cos_sin(spread(mix_ref[layer, 2]))
        cos3, sin3 = cos_sin(spread(mix_ref[layer, 3]))
        tans.append((sin2 / cos2, sin3 / cos3))
        cut = cos2 * cos2 * (cos3 * cos3) * (cos3 * cos3)
        scale = cut if scale is None else scale * cut
    angle = jnp.broadcast_to(phase_ref[1:2, :], (SUB, 128))
    for part in range(2):
        for bank in range(4):
            done = mix([in_ref[bank * 16 + i, part] for i in range(16)], tans[0][1])
            for i in range(16):
                work_ref[bank * 16 + i, part] = done[i]
    for i in range(16):
        re = mix([work_ref[bank * 16 + i, 0] for bank in range(4)], tans[0][0])
        im = mix([work_ref[bank * 16 + i, 1] for bank in range(4)], tans[0][0])
        for bank in range(4):
            cos, sin = cos_sin(in_ref[bank * 16 + i, 2] * angle)
            cos, sin = cos * scale, sin * scale
            u, v = re[bank], im[bank]
            re[bank], im[bank] = u * cos + v * sin, v * cos - u * sin
        re, im = mix(re, tans[1][0]), mix(im, tans[1][0])
        for bank in range(4):
            work_ref[bank * 16 + i, 0] = re[bank]
            work_ref[bank * 16 + i, 1] = im[bank]
    for part in range(2):
        for bank in range(4):
            done = mix([work_ref[bank * 16 + i, part] for i in range(16)], tans[1][1])
            for i in range(16):
                out_ref[bank * 16 + i, part] = done[i]


def last_kernel(mix_ref, in_ref, out_ref):
    lane_table, row_table, tan = tables(mix_ref, 1)
    parts = [[in_ref[b * 16 : b * 16 + 16, part].reshape(128, 128) for b in range(4)] for part in range(2)]
    for part, blocks in enumerate(within(parts, lane_table, row_table, tan)):
        for b in range(4):
            out_ref[part, b] = blocks[b]


VMEM = pl.BlockSpec(memory_space=pltpu.VMEM)
SMEM = pl.BlockSpec(memory_space=pltpu.SMEM)


def swap(values):
    return lax.all_to_all(values, ("bank", "lane"), split_axis=0, concat_axis=0, tiled=True)


def local(wave_parts, level_table, phase_angles, mix_angles):
    send = pl.pallas_call(
        first_kernel,
        out_shape=jax.ShapeDtypeStruct((64, 3, SUB, 128), F32),
        in_specs=[SMEM, VMEM, VMEM, VMEM],
        out_specs=VMEM,
        name="first",
    )(mix_angles, wave_parts, level_table, phase_angles)
    held = swap(send)
    back = pl.pallas_call(
        middle_kernel,
        out_shape=jax.ShapeDtypeStruct((64, 2, SUB, 128), F32),
        in_specs=[SMEM, VMEM, VMEM],
        out_specs=VMEM,
        scratch_shapes=[pltpu.VMEM((64, 2, SUB, 128), F32)],
        name="middle",
    )(mix_angles, phase_angles, held)
    mine = swap(back)
    return pl.pallas_call(
        last_kernel,
        out_shape=jax.ShapeDtypeStruct((2, 4, 128, 128), F32),
        in_specs=[SMEM, VMEM],
        out_specs=VMEM,
        name="last",
    )(mix_angles, mine)


def solution(mesh):
    placed = (
        P("site", ("bank", "lane"), None, None),
        P(("site", "bank", "lane"), None, None),
        P("site", None),
        P("site", None),
    )
    return jax.shard_map(
        local,
        mesh=mesh,
        in_specs=placed,
        out_specs=P("site", ("bank", "lane"), None, None),
        check_vma=False,
    )
```

```python
import jax
import jax.numpy as jnp
from jax import lax
from jax.experimental import pallas as pl
from jax.experimental.pallas import tpu as pltpu
from jax.sharding import PartitionSpec as P

SUB = 8
F32 = jnp.float32
BF16 = jnp.bfloat16

SIN = (0.9999999814442071, -0.16666657755521955, 0.008333210982283118, -0.00019834058585468524,
       2.734996203799263e-06, -2.21633008243829e-08)
COS = (0.9999999997000049, -0.4999999949621528, 0.04166665285119409, -0.0013888746708823352,
       2.4794608537121183e-05, -2.7380880775339007e-07, 1.8645524434398867e-09)


def series(z, terms):
    total = z * terms[-1] + terms[-2]
    for term in terms[-3::-1]:
        total = total * z + term
    return total


def cos_sin(x):
    z = x * x
    return series(z, COS), series(z, SIN) * x


def plane_table(cos, sin):
    row = lax.broadcasted_iota(jnp.int32, (128, 128), 0)
    col = lax.broadcasted_iota(jnp.int32, (128, 128), 1)
    apart = row ^ col
    table = None
    for bit in range(7):
        turned = jnp.where((row >> bit) & 1 == 1, -sin, sin)
        factor = jnp.where((apart >> bit) & 1 == 0, cos, turned)
        table = factor if table is None else table * factor
    return table


def halves(x):
    high = x.astype(BF16)
    return high, (x - high.astype(F32)).astype(BF16)


def dot(a, b):
    return lax.dot_general(a, b, (((1,), (0,)), ((), ())), preferred_element_type=F32)


def lane_weights(table):
    high, low = halves(table)
    both = jnp.concatenate([high, low], axis=1)
    return jnp.concatenate([both, both], axis=0)


def row_weights(table):
    high, low = halves(table)
    return jnp.concatenate(
        [jnp.concatenate([high, high], axis=1), jnp.concatenate([low, low], axis=1)], axis=0
    )


def along_lanes(x, weights):
    done = dot(jnp.concatenate(halves(x), axis=1), weights)
    return done[:, :128] + done[:, 128:]


def along_rows(x, weights):
    done = dot(weights, jnp.concatenate(halves(x), axis=0))
    return done[:128] + done[128:]


def mix(parts, tan):
    parts = list(parts)
    step = 1
    while step < len(parts):
        for i in range(len(parts)):
            if not i & step:
                u, v = parts[i], parts[i + step]
                parts[i], parts[i + step] = u - tan * v, v + tan * u
        step *= 2
    return parts


PHASE, TAN2, TAN3, NEXT2, NEXT3, SCALE, COS0, SIN0, COS1, SIN1, TILES = range(11)


def wide(tile):
    return jnp.broadcast_to(tile[0:1], (128, 128))


def first_kernel(mix_hbm, phase_hbm, wave_hbm, level_hbm, out_ref, aux_ref, mix_ref, phase_ref, wave_ref, done_ref, sems):
    small = [
        pltpu.make_async_copy(mix_hbm, mix_ref, sems.at[0]),
        pltpu.make_async_copy(phase_hbm, phase_ref, sems.at[1]),
    ]
    loads = []
    for copy in small:
        copy.start()
    for b in range(4):
        rows = pl.ds(b * 16, 16)
        pair = [
            pltpu.make_async_copy(level_hbm.at[b], out_ref.at[rows, 2], sems.at[2 + 2 * b]),
            pltpu.make_async_copy(wave_hbm.at[:, b], wave_ref.at[:, b], sems.at[3 + 2 * b]),
        ]
        for copy in pair:
            copy.start()
        loads.append(pair)
    for copy in small:
        copy.wait()
    trig = {}
    for layer in range(2):
        for group in range(4):
            angle = jnp.broadcast_to(mix_ref[layer : layer + 1, group : group + 1], (SUB, 128))
            trig[layer, group] = cos_sin(angle)
    tans = {key: sin / cos for key, (cos, sin) in trig.items() if key[1] > 1}
    scale = None
    for layer in range(2):
        cos2, cos3 = trig[layer, 2][0], trig[layer, 3][0]
        cut = cos2 * cos2 * (cos3 * cos3) * (cos3 * cos3)
        scale = cut if scale is None else scale * cut
    scale = scale * trig[0, 2][0] * trig[0, 2][0] * (trig[1, 2][0] * trig[1, 2][0])
    aux_ref[PHASE] = jnp.broadcast_to(phase_ref[1:2, :], (SUB, 128))
    aux_ref[TAN2], aux_ref[TAN3] = tans[0, 2], tans[0, 3]
    aux_ref[NEXT2], aux_ref[NEXT3] = tans[1, 2], tans[1, 3]
    aux_ref[SCALE] = scale
    aux_ref[COS0], aux_ref[SIN0] = trig[1, 0]
    aux_ref[COS1], aux_ref[SIN1] = trig[1, 1]
    lanes = lane_weights(plane_table(wide(trig[0, 0][0]), wide(trig[0, 0][1])))
    rows = row_weights(plane_table(wide(trig[0, 1][0]), wide(-trig[0, 1][1])))
    angle = phase_ref[0:1, :]
    for b in range(4):
        for copy in loads[b]:
            copy.wait()
        cos, sin = cos_sin(out_ref[b * 16 : b * 16 + 16, 2].reshape(128, 128) * angle)
        u, v = wave_ref[0, b].reshape(128, 128), wave_ref[1, b].reshape(128, 128)
        both = jnp.concatenate([u * cos + v * sin, v * cos - u * sin], axis=1)
        both = along_rows(both, rows)
        for part in range(2):
            x = along_lanes(both[:, part * 128 : part * 128 + 128], lanes)
            done_ref[part, b] = x.reshape(16, SUB, 128)
    tan = tans[0, 2]
    for part in range(2):
        for i in range(16):
            out = mix([done_ref[part, b, i] for b in range(4)], tan)
            for b in range(4):
                out_ref[b * 16 + i, part] = out[b]


def middle_kernel(aux_ref, in_ref, out_ref, work_ref):
    angle, scale = aux_ref[PHASE], aux_ref[SCALE]
    tan2, tan3, next2, next3 = aux_ref[TAN2], aux_ref[TAN3], aux_ref[NEXT2], aux_ref[NEXT3]
    for part in range(2):
        for bank in range(4):
            done = mix([in_ref[bank * 16 + i, part] for i in range(16)], tan3)
            for i in range(16):
                work_ref[bank * 16 + i, part] = done[i]
    for i in range(16):
        re = mix([work_ref[bank * 16 + i, 0] for bank in range(4)], tan2)
        im = mix([work_ref[bank * 16 + i, 1] for bank in range(4)], tan2)
        for bank in range(4):
            cos, sin = cos_sin(in_ref[bank * 16 + i, 2] * angle)
            cos, sin = cos * scale, sin * scale
            u, v = re[bank], im[bank]
            re[bank], im[bank] = u * cos + v * sin, v * cos - u * sin
        re, im = mix(re, next2), mix(im, next2)
        for bank in range(4):
            work_ref[bank * 16 + i, 0] = re[bank]
            work_ref[bank * 16 + i, 1] = im[bank]
    for part in range(2):
        for bank in range(4):
            done = mix([work_ref[bank * 16 + i, part] for i in range(16)], next3)
            for i in range(16):
                out_ref[bank * 16 + i, part] = done[i]


def last_kernel(aux_ref, in_ref, out_hbm, work_ref, out_ref, sems):
    tan = aux_ref[NEXT2]
    lanes = lane_weights(plane_table(wide(aux_ref[COS0]), wide(aux_ref[SIN0])))
    rows = row_weights(plane_table(wide(aux_ref[COS1]), wide(-aux_ref[SIN1])))
    for part in range(2):
        for i in range(16):
            out = mix([in_ref[b * 16 + i, part] for b in range(4)], tan)
            for b in range(4):
                work_ref[part, b, i] = out[b]
    copies = []
    for b in range(4):
        both = jnp.concatenate([work_ref[part, b].reshape(128, 128) for part in range(2)], axis=1)
        both = along_rows(both, rows)
        for part in range(2):
            out_ref[part, b] = along_lanes(both[:, part * 128 : part * 128 + 128], lanes)
        copy = pltpu.make_async_copy(out_ref.at[:, b], out_hbm.at[:, b], sems.at[b])
        copy.start()
        copies.append(copy)
    for copy in copies:
        copy.wait()


VMEM = pl.BlockSpec(memory_space=pltpu.VMEM)
HBM = pl.BlockSpec(memory_space=pltpu.HBM)
ROOM = pltpu.CompilerParams(vmem_limit_bytes=12 << 20)


def swap(values):
    return lax.all_to_all(values, ("bank", "lane"), split_axis=0, concat_axis=0, tiled=True)


def local(wave_parts, level_table, phase_angles, mix_angles):
    send, aux = pl.pallas_call(
        first_kernel,
        out_shape=(
            jax.ShapeDtypeStruct((64, 3, SUB, 128), F32),
            jax.ShapeDtypeStruct((TILES, SUB, 128), F32),
        ),
        in_specs=[HBM] * 4,
        out_specs=(VMEM, VMEM),
        scratch_shapes=[
            pltpu.VMEM((2, 4), F32),
            pltpu.VMEM((2, 128), F32),
            pltpu.VMEM((2, 4, 16, SUB, 128), F32),
            pltpu.VMEM((2, 4, 16, SUB, 128), F32),
            pltpu.SemaphoreType.DMA((10,)),
        ],
        compiler_params=ROOM,
        name="first",
    )(*(pltpu.with_memory_space_constraint(v, pltpu.HBM) for v in (mix_angles, phase_angles, wave_parts.reshape(2, 4, 16, SUB, 128), level_table.reshape(4, 16, SUB, 128))))
    held = swap(send)
    back = pl.pallas_call(
        middle_kernel,
        out_shape=jax.ShapeDtypeStruct((64, 2, SUB, 128), F32),
        in_specs=[VMEM, VMEM],
        out_specs=VMEM,
        scratch_shapes=[pltpu.VMEM((64, 2, SUB, 128), F32)],
        compiler_params=ROOM,
        name="middle",
    )(aux, held)
    mine = swap(back)
    return pl.pallas_call(
        last_kernel,
        out_shape=jax.ShapeDtypeStruct((2, 4, 128, 128), F32),
        in_specs=[VMEM, VMEM],
        out_specs=HBM,
        scratch_shapes=[
            pltpu.VMEM((2, 4, 16, SUB, 128), F32),
            pltpu.VMEM((2, 4, 128, 128), F32),
            pltpu.SemaphoreType.DMA((4,)),
        ],
        compiler_params=ROOM,
        name="last",
    )(aux, mine)


def solution(mesh):
    placed = (
        P("site", ("bank", "lane"), None, None),
        P(("site", "bank", "lane"), None, None),
        P("site", None),
        P("site", None),
    )
    return jax.shard_map(
        local,
        mesh=mesh,
        in_specs=placed,
        out_specs=P("site", ("bank", "lane"), None, None),
        check_vma=False,
    )
```

```python
import jax
import jax.numpy as jnp
from jax import lax
from jax.experimental import pallas as pl
from jax.experimental.pallas import tpu as pltpu
from jax.sharding import PartitionSpec as P

SUB = 8
ORDER = [
    (bank + 2) % 4 * 16 + (y + 4) % 8 * 2 + 1 - core
    for y in range(8)
    for core in range(2)
    for bank in range(4)
]
PLACE = [ORDER.index(k) for k in range(64)]
F32 = jnp.float32
BF16 = jnp.bfloat16

SIN = (0.9999999814442071, -0.16666657755521955, 0.008333210982283118, -0.00019834058585468524,
       2.734996203799263e-06, -2.21633008243829e-08)
COS = (0.9999999997000049, -0.4999999949621528, 0.04166665285119409, -0.0013888746708823352,
       2.4794608537121183e-05, -2.7380880775339007e-07, 1.8645524434398867e-09)


def series(z, terms):
    total = z * terms[-1] + terms[-2]
    for term in terms[-3::-1]:
        total = total * z + term
    return total


def cos_sin(x):
    z = x * x
    return series(z, COS), series(z, SIN) * x


def plane_table(cos, sin):
    row = lax.broadcasted_iota(jnp.int32, (128, 128), 0)
    col = lax.broadcasted_iota(jnp.int32, (128, 128), 1)
    apart = row ^ col
    table = None
    for bit in range(7):
        turned = jnp.where((row >> bit) & 1 == 1, -sin, sin)
        factor = jnp.where((apart >> bit) & 1 == 0, cos, turned)
        table = factor if table is None else table * factor
    return table


def halves(x):
    high = x.astype(BF16)
    return high, (x - high.astype(F32)).astype(BF16)


def dot(a, b):
    return lax.dot_general(a, b, (((1,), (0,)), ((), ())), preferred_element_type=F32)


def lane_weights(table):
    high, low = halves(table)
    both = jnp.concatenate([high, low], axis=1)
    return jnp.concatenate([both, both], axis=0)


def row_weights(table):
    high, low = halves(table)
    return jnp.concatenate(
        [jnp.concatenate([high, high], axis=1), jnp.concatenate([low, low], axis=1)], axis=0
    )


def along_lanes(x, weights):
    done = dot(jnp.concatenate(halves(x), axis=1), weights)
    return done[:, :128] + done[:, 128:]


def along_rows(x, weights):
    done = dot(weights, jnp.concatenate(halves(x), axis=0))
    return done[:128] + done[128:]


def mix(parts, tan):
    parts = list(parts)
    step = 1
    while step < len(parts):
        for i in range(len(parts)):
            if not i & step:
                u, v = parts[i], parts[i + step]
                parts[i], parts[i + step] = u - tan * v, v + tan * u
        step *= 2
    return parts


PHASE, TAN2, TAN3, NEXT2, NEXT3, SCALE, COS0, SIN0, COS1, SIN1, TILES = range(11)


def wide(tile):
    return jnp.broadcast_to(tile[0:1], (128, 128))


def first_kernel(mix_hbm, phase_hbm, wave_hbm, level_hbm, out_ref, aux_ref, mix_ref, phase_ref, wave_ref, done_ref, sems):
    small = [
        pltpu.make_async_copy(mix_hbm, mix_ref, sems.at[0]),
        pltpu.make_async_copy(phase_hbm, phase_ref, sems.at[1]),
    ]
    loads = []
    for copy in small:
        copy.start()
    for b in range(4):
        rows = pl.ds(b * 16, 16)
        pair = [
            pltpu.make_async_copy(level_hbm.at[b], out_ref.at[rows, 2], sems.at[2 + 2 * b]),
            pltpu.make_async_copy(wave_hbm.at[:, b], wave_ref.at[:, b], sems.at[3 + 2 * b]),
        ]
        for copy in pair:
            copy.start()
        loads.append(pair)
    for copy in small:
        copy.wait()
    trig = {}
    for layer in range(2):
        for group in range(4):
            angle = jnp.broadcast_to(mix_ref[layer : layer + 1, group : group + 1], (SUB, 128))
            trig[layer, group] = cos_sin(angle)
    tans = {key: sin / cos for key, (cos, sin) in trig.items() if key[1] > 1}
    scale = None
    for layer in range(2):
        cos2, cos3 = trig[layer, 2][0], trig[layer, 3][0]
        cut = cos2 * cos2 * (cos3 * cos3) * (cos3 * cos3)
        scale = cut if scale is None else scale * cut
    scale = scale * trig[0, 2][0] * trig[0, 2][0] * (trig[1, 2][0] * trig[1, 2][0])
    aux_ref[PHASE] = jnp.broadcast_to(phase_ref[1:2, :], (SUB, 128))
    aux_ref[TAN2], aux_ref[TAN3] = tans[0, 2], tans[0, 3]
    aux_ref[NEXT2], aux_ref[NEXT3] = tans[1, 2], tans[1, 3]
    aux_ref[SCALE] = scale
    aux_ref[COS0], aux_ref[SIN0] = trig[1, 0]
    aux_ref[COS1], aux_ref[SIN1] = trig[1, 1]
    lanes = lane_weights(plane_table(wide(trig[0, 0][0]), wide(trig[0, 0][1])))
    rows = row_weights(plane_table(wide(trig[0, 1][0]), wide(-trig[0, 1][1])))
    angle = phase_ref[0:1, :]
    for pair in loads:
        for copy in pair:
            copy.wait()
    for b in range(4):
        cos, sin = cos_sin(out_ref[b * 16 : b * 16 + 16, 2].reshape(128, 128) * angle)
        u, v = wave_ref[0, b].reshape(128, 128), wave_ref[1, b].reshape(128, 128)
        both = jnp.concatenate([u * cos + v * sin, v * cos - u * sin], axis=1)
        both = along_rows(both, rows)
        for part in range(2):
            x = both[:, part * 128 : part * 128 + 128]
            x = along_lanes(x, lanes)
            done_ref[part, b] = x.reshape(16, SUB, 128)
    tan = tans[0, 2]
    for part in range(2):
        for i in range(16):
            out = mix([done_ref[part, b, i] for b in range(4)], tan)
            for b in range(4):
                out_ref[b * 16 + i, part] = out[b]


def middle_kernel(aux_ref, in_ref, out_ref, work_ref):
    angle, scale = aux_ref[PHASE], aux_ref[SCALE]
    tan2, tan3, next2, next3 = aux_ref[TAN2], aux_ref[TAN3], aux_ref[NEXT2], aux_ref[NEXT3]
    for part in range(2):
        for bank in range(4):
            done = mix([in_ref[PLACE[bank * 16 + i], part] for i in range(16)], tan3)
            for i in range(16):
                work_ref[bank * 16 + i, part] = done[i]
    for i in range(16):
        re = mix([work_ref[bank * 16 + i, 0] for bank in range(4)], tan2)
        im = mix([work_ref[bank * 16 + i, 1] for bank in range(4)], tan2)
        for bank in range(4):
            cos, sin = cos_sin(in_ref[PLACE[bank * 16 + i], 2] * angle)
            cos, sin = cos * scale, sin * scale
            u, v = re[bank], im[bank]
            re[bank], im[bank] = u * cos + v * sin, v * cos - u * sin
        re, im = mix(re, next2), mix(im, next2)
        for bank in range(4):
            work_ref[bank * 16 + i, 0] = re[bank]
            work_ref[bank * 16 + i, 1] = im[bank]
    for part in range(2):
        for bank in range(4):
            done = mix([work_ref[bank * 16 + i, part] for i in range(16)], next3)
            for i in range(16):
                out_ref[PLACE[bank * 16 + i], part] = done[i]


def last_kernel(aux_ref, in_ref, out_hbm, work_ref, out_ref, sems):
    tan = aux_ref[NEXT2]
    lanes = lane_weights(plane_table(wide(aux_ref[COS0]), wide(aux_ref[SIN0])))
    rows = row_weights(plane_table(wide(aux_ref[COS1]), wide(-aux_ref[SIN1])))
    for part in range(2):
        for i in range(16):
            out = mix([in_ref[b * 16 + i, part] for b in range(4)], tan)
            for b in range(4):
                work_ref[part, b, i] = out[b]
    copies = []
    for b in range(4):
        both = jnp.concatenate([work_ref[part, b].reshape(128, 128) for part in range(2)], axis=1)
        both = along_rows(both, rows)
        for part in range(2):
            out_ref[part, b] = along_lanes(both[:, part * 128 : part * 128 + 128], lanes)
        copy = pltpu.make_async_copy(out_ref.at[:, b], out_hbm.at[:, b], sems.at[b])
        copy.start()
        copies.append(copy)
    for copy in copies:
        copy.wait()


VMEM = pl.BlockSpec(memory_space=pltpu.VMEM)
HBM = pl.BlockSpec(memory_space=pltpu.HBM)
ROOM = pltpu.CompilerParams(vmem_limit_bytes=12 << 20)


def swap(values):
    return lax.all_to_all(
        values, ("bank", "lane"), split_axis=0, concat_axis=0, axis_index_groups=[ORDER], tiled=True
    )


def local(wave_parts, level_table, phase_angles, mix_angles):
    send, aux = pl.pallas_call(
        first_kernel,
        out_shape=(
            jax.ShapeDtypeStruct((64, 3, SUB, 128), F32),
            jax.ShapeDtypeStruct((TILES, SUB, 128), F32),
        ),
        in_specs=[HBM] * 4,
        out_specs=(VMEM, VMEM),
        scratch_shapes=[
            pltpu.VMEM((2, 4), F32),
            pltpu.VMEM((2, 128), F32),
            pltpu.VMEM((2, 4, 16, SUB, 128), F32),
            pltpu.VMEM((2, 4, 16, SUB, 128), F32),
            pltpu.SemaphoreType.DMA((10,)),
        ],
        compiler_params=ROOM,
        name="first",
    )(*(pltpu.with_memory_space_constraint(v, pltpu.HBM) for v in (mix_angles, phase_angles, wave_parts.reshape(2, 4, 16, SUB, 128), level_table.reshape(4, 16, SUB, 128))))
    held = swap(send)
    back = pl.pallas_call(
        middle_kernel,
        out_shape=jax.ShapeDtypeStruct((64, 2, SUB, 128), F32),
        in_specs=[VMEM, VMEM],
        out_specs=VMEM,
        scratch_shapes=[pltpu.VMEM((64, 2, SUB, 128), F32)],
        compiler_params=ROOM,
        name="middle",
    )(aux, held)
    mine = swap(back)
    return pl.pallas_call(
        last_kernel,
        out_shape=jax.ShapeDtypeStruct((2, 4, 128, 128), F32),
        in_specs=[VMEM, VMEM],
        out_specs=HBM,
        scratch_shapes=[
            pltpu.VMEM((2, 4, 16, SUB, 128), F32),
            pltpu.VMEM((2, 4, 128, 128), F32),
            pltpu.SemaphoreType.DMA((4,)),
        ],
        compiler_params=ROOM,
        name="last",
    )(aux, mine)


def solution(mesh):
    placed = (
        P("site", ("bank", "lane"), None, None),
        P(("site", "bank", "lane"), None, None),
        P("site", None),
        P("site", None),
    )
    return jax.shard_map(
        local,
        mesh=mesh,
        in_specs=placed,
        out_specs=P("site", ("bank", "lane"), None, None),
        check_vma=False,
    )
```

```python
import jax
import jax.numpy as jnp
from jax import lax
from jax.experimental import pallas as pl
from jax.experimental.pallas import tpu as pltpu
from jax.sharding import PartitionSpec as P

SUB = 8
ORDER = [
    bank * 16 + (y + 4) % 8 * 2 + 1 - core for y in range(8) for core in range(2) for bank in (2, 0, 3, 1)
]
PLACE = [ORDER.index(k) for k in range(64)]
F32 = jnp.float32
BF16 = jnp.bfloat16

SIN = (0.9999999814442071, -0.16666657755521955, 0.008333210982283118, -0.00019834058585468524,
       2.734996203799263e-06, -2.21633008243829e-08)
COS = (0.9999999997000049, -0.4999999949621528, 0.04166665285119409, -0.0013888746708823352,
       2.4794608537121183e-05, -2.7380880775339007e-07, 1.8645524434398867e-09)


def series(z, terms):
    total = z * terms[-1] + terms[-2]
    for term in terms[-3::-1]:
        total = total * z + term
    return total


def cos_sin(x):
    z = x * x
    return series(z, COS), series(z, SIN) * x


def plane_table(cos, sin, bits):
    row = lax.broadcasted_iota(jnp.int32, (128, 128), 0)
    col = lax.broadcasted_iota(jnp.int32, (128, 128), 1)
    apart = row ^ col
    table = jnp.where(apart >> bits == 0, 1.0, 0.0).astype(F32)
    for bit in range(bits):
        turned = jnp.where((row >> bit) & 1 == 1, -sin, sin)
        table = table * jnp.where((apart >> bit) & 1 == 0, cos, turned)
    return table


def halves(x):
    high = x.astype(BF16)
    return high, (x - high.astype(F32)).astype(BF16)


def dot(a, b):
    return lax.dot_general(a, b, (((1,), (0,)), ((), ())), preferred_element_type=F32)


def lane_weights(table):
    both = jnp.concatenate(halves(table), axis=1)
    return jnp.concatenate([both, both], axis=0)


def row_weights(table):
    return jnp.concatenate([jnp.concatenate([half, half], axis=1) for half in halves(table)], axis=0)


def within(parts, lanes, rows):
    both = jnp.concatenate([jnp.concatenate(tiles, axis=0) for tiles in parts], axis=1)
    both = dot(rows, jnp.concatenate(halves(both), axis=0))
    both = both[:128] + both[128:]
    out = []
    for part in range(2):
        done = dot(jnp.concatenate(halves(both[:, part * 128 : part * 128 + 128]), axis=1), lanes)
        done = done[:, :128] + done[:, 128:]
        out.append([done[i * SUB : i * SUB + SUB] for i in range(16)])
    return out


def mix(parts, tan):
    parts = list(parts)
    step = 1
    while step < len(parts):
        for i in range(len(parts)):
            if not i & step:
                u, v = parts[i], parts[i + step]
                parts[i], parts[i + step] = u - tan * v, v + tan * u
        step *= 2
    return parts


PHASE, SCALE, TAN2, TAN3, NEXT1, NEXT2, NEXT3, TILES = range(8)


def wide(tile):
    return jnp.broadcast_to(tile[0:1], (128, 128))


def trig_of(mix_ref, layer, group):
    return cos_sin(jnp.broadcast_to(mix_ref[layer : layer + 1, group : group + 1], (SUB, 128)))


def share(mix_ref, phase_ref, aux_ref, lanes_ref, rows_ref):
    scale, tans = None, {}
    for layer in range(2):
        trig = [trig_of(mix_ref, layer, group) for group in range(4)]
        for group, (cos, sin) in enumerate(trig):
            tans[layer, group] = sin / cos
        cut = trig[1][0] * trig[2][0] * trig[3][0]
        cut = cut * cut
        cut = cut * cut
        scale = cut if scale is None else scale * cut
        lanes_ref[layer] = lane_weights(plane_table(wide(trig[0][0]), wide(trig[0][1]), 7))
        rows_ref[layer] = row_weights(plane_table(wide(trig[1][0]), wide(-trig[1][1]), 3))
    aux_ref[PHASE] = jnp.broadcast_to(phase_ref[1:2, :], (SUB, 128))
    aux_ref[SCALE] = scale
    aux_ref[TAN2], aux_ref[TAN3] = tans[0, 2], tans[0, 3]
    aux_ref[NEXT1], aux_ref[NEXT2], aux_ref[NEXT3] = tans[1, 1], tans[1, 2], tans[1, 3]
    return tans[0, 1], tans[0, 2]


def first_kernel(
    mix_hbm, phase_hbm, wave_hbm, level_hbm, out_ref, aux_ref, lanes_ref, rows_ref, mix_ref, phase_ref, wave_ref, sems
):
    small = [
        pltpu.make_async_copy(mix_hbm, mix_ref, sems.at[0]),
        pltpu.make_async_copy(phase_hbm, phase_ref, sems.at[1]),
    ]
    loads = []
    for copy in small:
        copy.start()
    for b in range(4):
        pair = [
            pltpu.make_async_copy(level_hbm.at[b], out_ref.at[pl.ds(b * 16, 16), 2], sems.at[2 + 2 * b]),
            pltpu.make_async_copy(wave_hbm.at[:, b], wave_ref.at[:, b], sems.at[3 + 2 * b]),
        ]
        for copy in pair:
            copy.start()
        loads.append(pair)
    for copy in small:
        copy.wait()
    tans = share(mix_ref, phase_ref, aux_ref, lanes_ref, rows_ref)
    angle = jnp.broadcast_to(phase_ref[0:1, :], (SUB, 128))
    for b in range(4):
        for copy in loads[b]:
            copy.wait()
        re, im = [], []
        for i in range(16):
            cos, sin = cos_sin(out_ref[b * 16 + i, 2] * angle)
            u, v = wave_ref[0, b, i], wave_ref[1, b, i]
            re.append(u * cos + v * sin)
            im.append(v * cos - u * sin)
        for part, tiles in enumerate((re, im)):
            for i, tile in enumerate(mix(tiles, tans[0])):
                wave_ref[part, b, i] = tile
    for part in range(2):
        for i in range(16):
            for b, tile in enumerate(mix([wave_ref[part, b, i] for b in range(4)], tans[1])):
                out_ref[b * 16 + i, part] = tile


def middle_kernel(aux_ref, lanes_ref, rows_ref, in_ref, out_ref, work_ref):
    angle, scale = aux_ref[PHASE], aux_ref[SCALE]
    tan2, tan3, next2, next3 = aux_ref[TAN2], aux_ref[TAN3], aux_ref[NEXT2], aux_ref[NEXT3]
    lanes, rows = lanes_ref[0], rows_ref[0]
    for bank in range(4):
        parts = [mix([in_ref[PLACE[bank * 16 + i], part] for i in range(16)], tan3) for part in range(2)]
        parts = within(parts, lanes, rows)
        for part in range(2):
            for i in range(16):
                work_ref[bank, i, part] = parts[part][i]
    for i in range(16):
        re = mix([work_ref[bank, i, 0] for bank in range(4)], tan2)
        im = mix([work_ref[bank, i, 1] for bank in range(4)], tan2)
        for bank in range(4):
            cos, sin = cos_sin(in_ref[PLACE[bank * 16 + i], 2] * angle)
            cos, sin = cos * scale, sin * scale
            u, v = re[bank], im[bank]
            re[bank], im[bank] = u * cos + v * sin, v * cos - u * sin
        re, im = mix(re, next2), mix(im, next2)
        for bank in range(4):
            work_ref[bank, i, 0] = re[bank]
            work_ref[bank, i, 1] = im[bank]
    lanes, rows = lanes_ref[1], rows_ref[1]
    for bank in range(4):
        parts = within([[work_ref[bank, i, part] for i in range(16)] for part in range(2)], lanes, rows)
        for part in range(2):
            for i, tile in enumerate(mix(parts[part], next3)):
                out_ref[PLACE[bank * 16 + i], part] = tile


def last_kernel(aux_ref, in_ref, out_hbm, work_ref, out_ref, sems):
    next1, next2 = aux_ref[NEXT1], aux_ref[NEXT2]
    for part in range(2):
        for i in range(16):
            for b, tile in enumerate(mix([in_ref[b * 16 + i, part] for b in range(4)], next2)):
                work_ref[part, b, i] = tile
    copies = []
    for b in range(4):
        for part in range(2):
            for i, tile in enumerate(mix([work_ref[part, b, i] for i in range(16)], next1)):
                out_ref[part, b, i] = tile
        copy = pltpu.make_async_copy(out_ref.at[:, b], out_hbm.at[:, b], sems.at[b])
        copy.start()
        copies.append(copy)
    for copy in copies:
        copy.wait()


VMEM = pl.BlockSpec(memory_space=pltpu.VMEM)
HBM = pl.BlockSpec(memory_space=pltpu.HBM)
ROOM = pltpu.CompilerParams(vmem_limit_bytes=12 << 20)


def swap(values):
    return lax.all_to_all(
        values, ("bank", "lane"), split_axis=0, concat_axis=0, axis_index_groups=[ORDER], tiled=True
    )


def local(wave_parts, level_table, phase_angles, mix_angles):
    wave_parts, level_table, phase_angles, mix_angles = (
        pltpu.with_memory_space_constraint(v, pltpu.HBM)
        for v in (
            wave_parts.reshape(2, 4, 16, SUB, 128),
            level_table.reshape(4, 16, SUB, 128),
            phase_angles,
            mix_angles,
        )
    )
    send, aux, lanes, rows = pl.pallas_call(
        first_kernel,
        out_shape=(
            jax.ShapeDtypeStruct((64, 3, SUB, 128), F32),
            jax.ShapeDtypeStruct((TILES, SUB, 128), F32),
            jax.ShapeDtypeStruct((2, 256, 256), BF16),
            jax.ShapeDtypeStruct((2, 256, 256), BF16),
        ),
        in_specs=[HBM] * 4,
        out_specs=(VMEM,) * 4,
        scratch_shapes=[
            pltpu.VMEM((2, 4), F32),
            pltpu.VMEM((2, 128), F32),
            pltpu.VMEM((2, 4, 16, SUB, 128), F32),
            pltpu.SemaphoreType.DMA((10,)),
        ],
        compiler_params=ROOM,
        name="first",
    )(mix_angles, phase_angles, wave_parts, level_table)
    held = swap(send)
    back = pl.pallas_call(
        middle_kernel,
        out_shape=jax.ShapeDtypeStruct((64, 2, SUB, 128), F32),
        in_specs=[VMEM] * 4,
        out_specs=VMEM,
        scratch_shapes=[pltpu.VMEM((4, 16, 2, SUB, 128), F32)],
        compiler_params=ROOM,
        name="middle",
    )(aux, lanes, rows, held)
    mine = swap(back)
    out = pl.pallas_call(
        last_kernel,
        out_shape=jax.ShapeDtypeStruct((2, 4, 16, SUB, 128), F32),
        in_specs=[VMEM, VMEM],
        out_specs=HBM,
        scratch_shapes=[
            pltpu.VMEM((2, 4, 16, SUB, 128), F32),
            pltpu.VMEM((2, 4, 16, SUB, 128), F32),
            pltpu.SemaphoreType.DMA((4,)),
        ],
        compiler_params=ROOM,
        name="last",
    )(aux, mine)
    return out.reshape(2, 4, 128, 128)


def solution(mesh):
    placed = (
        P("site", ("bank", "lane"), None, None),
        P(("site", "bank", "lane"), None, None),
        P("site", None),
        P("site", None),
    )
    return jax.shard_map(
        local,
        mesh=mesh,
        in_specs=placed,
        out_specs=P("site", ("bank", "lane"), None, None),
        check_vma=False,
    )
```

```python
import jax
import jax.numpy as jnp
from jax import lax
from jax.experimental import pallas as pl
from jax.experimental.pallas import tpu as pltpu
from jax.sharding import PartitionSpec as P

SUB = 8
ORDER = [
    bank * 16 + (y + 4) % 8 * 2 + 1 - core for y in range(8) for core in range(2) for bank in (2, 0, 3, 1)
]
PLACE = [ORDER.index(k) for k in range(64)]
F32 = jnp.float32
BF16 = jnp.bfloat16

SIN = (0.9999999814442071, -0.16666657755521955, 0.008333210982283118, -0.00019834058585468524,
       2.734996203799263e-06, -2.21633008243829e-08)
COS = (0.9999999997000049, -0.4999999949621528, 0.04166665285119409, -0.0013888746708823352,
       2.4794608537121183e-05, -2.7380880775339007e-07, 1.8645524434398867e-09)


def series(z, terms):
    total = z * terms[-1] + terms[-2]
    for term in terms[-3::-1]:
        total = total * z + term
    return total


def cos_sin(x):
    z = x * x
    return series(z, COS), series(z, SIN) * x


def bit_factor(cos, sin, column, bit, row_bit):
    at = (column >> bit) & 1
    if isinstance(row_bit, bool):
        return jnp.where(at == row_bit, cos, -sin if row_bit else sin)
    return jnp.where(at == row_bit, cos, jnp.where(row_bit == 1, -sin, sin))


def low_table(cos, sin):
    row = lax.broadcasted_iota(jnp.int32, (SUB, 128), 0)
    column = lax.broadcasted_iota(jnp.int32, (SUB, 128), 1)
    tile = None
    for bit in range(3):
        factor = bit_factor(cos, sin, column, bit, (row >> bit) & 1)
        tile = factor if tile is None else tile * factor
    return tile


def lane_table(cos, sin):
    column = lax.broadcasted_iota(jnp.int32, (SUB, 128), 1)
    tiles = [low_table(cos, sin)]
    for bit in range(3, 7):
        pair = [bit_factor(cos, sin, column, bit, at) for at in (False, True)]
        tiles = [tile * factor for factor in pair for tile in tiles]
    return jnp.concatenate(tiles, axis=0)


def row_table(cos, sin):
    tile = low_table(cos, -sin)
    group = lax.broadcasted_iota(jnp.int32, (SUB, 128), 1) >> 3
    return jnp.concatenate([jnp.where(group == i, tile, 0.0) for i in range(16)], axis=0)


def halves(x):
    high = x.astype(BF16)
    return high, (x - high.astype(F32)).astype(BF16)


def dot(a, b):
    return lax.dot_general(a, b, (((1,), (0,)), ((), ())), preferred_element_type=F32)


def lane_weights(table):
    both = jnp.concatenate(halves(table), axis=1)
    return jnp.concatenate([both, both], axis=0)


def row_weights(table):
    return jnp.concatenate([jnp.concatenate([half, half], axis=1) for half in halves(table)], axis=0)


def within(parts, lanes, rows):
    both = jnp.concatenate([jnp.concatenate(tiles, axis=0) for tiles in parts], axis=1)
    both = dot(rows, jnp.concatenate(halves(both), axis=0))
    both = both[:128] + both[128:]
    out = []
    for part in range(2):
        done = dot(jnp.concatenate(halves(both[:, part * 128 : part * 128 + 128]), axis=1), lanes)
        done = done[:, :128] + done[:, 128:]
        out.append([done[i * SUB : i * SUB + SUB] for i in range(16)])
    return out


def mix(parts, tan):
    parts = list(parts)
    step = 1
    while step < len(parts):
        for i in range(len(parts)):
            if not i & step:
                u, v = parts[i], parts[i + step]
                parts[i], parts[i + step] = u - tan * v, v + tan * u
        step *= 2
    return parts


PHASE, SCALE, TAN2, TAN3, NEXT1, NEXT2, NEXT3, TILES = range(8)


def trig_of(mix_ref, layer, group):
    return cos_sin(jnp.broadcast_to(mix_ref[layer : layer + 1, group : group + 1], (SUB, 128)))


def share(mix_ref, phase_ref, aux_ref, lanes_ref, rows_ref):
    scale, tans = None, {}
    for layer in range(2):
        trig = [trig_of(mix_ref, layer, group) for group in range(4)]
        for group, (cos, sin) in enumerate(trig):
            tans[layer, group] = sin / cos
        cut = trig[1][0] * trig[2][0] * trig[3][0]
        cut = cut * cut
        cut = cut * cut
        scale = cut if scale is None else scale * cut
        lanes_ref[layer] = lane_weights(lane_table(*trig[0]))
        rows_ref[layer] = row_weights(row_table(*trig[1]))
    aux_ref[PHASE] = jnp.broadcast_to(phase_ref[1:2, :], (SUB, 128))
    aux_ref[SCALE] = scale
    aux_ref[TAN2], aux_ref[TAN3] = tans[0, 2], tans[0, 3]
    aux_ref[NEXT1], aux_ref[NEXT2], aux_ref[NEXT3] = tans[1, 1], tans[1, 2], tans[1, 3]
    return tans[0, 1], tans[0, 2]


def first_kernel(
    mix_hbm, phase_hbm, wave_hbm, level_hbm, out_ref, aux_ref, lanes_ref, rows_ref, mix_ref, phase_ref, wave_ref, sems
):
    small = [
        pltpu.make_async_copy(mix_hbm, mix_ref, sems.at[0]),
        pltpu.make_async_copy(phase_hbm, phase_ref, sems.at[1]),
    ]
    loads = []
    for copy in small:
        copy.start()
    for b in range(4):
        pair = [
            pltpu.make_async_copy(level_hbm.at[b], out_ref.at[pl.ds(b * 16, 16), 2], sems.at[2 + 2 * b]),
            pltpu.make_async_copy(wave_hbm.at[:, b], wave_ref.at[:, b], sems.at[3 + 2 * b]),
        ]
        for copy in pair:
            copy.start()
        loads.append(pair)
    for copy in small:
        copy.wait()
    tans = share(mix_ref, phase_ref, aux_ref, lanes_ref, rows_ref)
    angle = jnp.broadcast_to(phase_ref[0:1, :], (SUB, 128))
    for b in range(4):
        for copy in loads[b]:
            copy.wait()
        re, im = [], []
        for i in range(16):
            cos, sin = cos_sin(out_ref[b * 16 + i, 2] * angle)
            u, v = wave_ref[0, b, i], wave_ref[1, b, i]
            re.append(u * cos + v * sin)
            im.append(v * cos - u * sin)
        for part, tiles in enumerate((re, im)):
            for i, tile in enumerate(mix(tiles, tans[0])):
                wave_ref[part, b, i] = tile
    for part in range(2):
        for i in range(16):
            for b, tile in enumerate(mix([wave_ref[part, b, i] for b in range(4)], tans[1])):
                out_ref[b * 16 + i, part] = tile


def middle_kernel(aux_ref, lanes_ref, rows_ref, in_ref, out_ref, work_ref):
    angle, scale = aux_ref[PHASE], aux_ref[SCALE]
    tan2, tan3, next2, next3 = aux_ref[TAN2], aux_ref[TAN3], aux_ref[NEXT2], aux_ref[NEXT3]
    lanes, rows = lanes_ref[0], rows_ref[0]
    for bank in range(4):
        parts = [mix([in_ref[PLACE[bank * 16 + i], part] for i in range(16)], tan3) for part in range(2)]
        parts = within(parts, lanes, rows)
        for part in range(2):
            for i in range(16):
                work_ref[bank, i, part] = parts[part][i]
    for i in range(16):
        re = mix([work_ref[bank, i, 0] for bank in range(4)], tan2)
        im = mix([work_ref[bank, i, 1] for bank in range(4)], tan2)
        for bank in range(4):
            cos, sin = cos_sin(in_ref[PLACE[bank * 16 + i], 2] * angle)
            cos, sin = cos * scale, sin * scale
            u, v = re[bank], im[bank]
            re[bank], im[bank] = u * cos + v * sin, v * cos - u * sin
        re, im = mix(re, next2), mix(im, next2)
        for bank in range(4):
            work_ref[bank, i, 0] = re[bank]
            work_ref[bank, i, 1] = im[bank]
    lanes, rows = lanes_ref[1], rows_ref[1]
    for bank in range(4):
        parts = within([[work_ref[bank, i, part] for i in range(16)] for part in range(2)], lanes, rows)
        for part in range(2):
            for i, tile in enumerate(mix(parts[part], next3)):
                out_ref[PLACE[bank * 16 + i], part] = tile


def last_kernel(aux_ref, in_ref, out_hbm, work_ref, out_ref, sems):
    next1, next2 = aux_ref[NEXT1], aux_ref[NEXT2]
    for part in range(2):
        for i in range(16):
            for b, tile in enumerate(mix([in_ref[b * 16 + i, part] for b in range(4)], next2)):
                work_ref[part, b, i] = tile
    copies = []
    for b in range(4):
        for part in range(2):
            for i, tile in enumerate(mix([work_ref[part, b, i] for i in range(16)], next1)):
                out_ref[part, b, i] = tile
        copy = pltpu.make_async_copy(out_ref.at[:, b], out_hbm.at[:, b], sems.at[b])
        copy.start()
        copies.append(copy)
    for copy in copies:
        copy.wait()


VMEM = pl.BlockSpec(memory_space=pltpu.VMEM)
HBM = pl.BlockSpec(memory_space=pltpu.HBM)
ROOM = pltpu.CompilerParams(vmem_limit_bytes=12 << 20)


def swap(values):
    return lax.all_to_all(
        values, ("bank", "lane"), split_axis=0, concat_axis=0, axis_index_groups=[ORDER], tiled=True
    )


def local(wave_parts, level_table, phase_angles, mix_angles):
    wave_parts, level_table, phase_angles, mix_angles = (
        pltpu.with_memory_space_constraint(v, pltpu.HBM)
        for v in (
            wave_parts.reshape(2, 4, 16, SUB, 128),
            level_table.reshape(4, 16, SUB, 128),
            phase_angles,
            mix_angles,
        )
    )
    send, aux, lanes, rows = pl.pallas_call(
        first_kernel,
        out_shape=(
            jax.ShapeDtypeStruct((64, 3, SUB, 128), F32),
            jax.ShapeDtypeStruct((TILES, SUB, 128), F32),
            jax.ShapeDtypeStruct((2, 256, 256), BF16),
            jax.ShapeDtypeStruct((2, 256, 256), BF16),
        ),
        in_specs=[HBM] * 4,
        out_specs=(VMEM,) * 4,
        scratch_shapes=[
            pltpu.VMEM((2, 4), F32),
            pltpu.VMEM((2, 128), F32),
            pltpu.VMEM((2, 4, 16, SUB, 128), F32),
            pltpu.SemaphoreType.DMA((10,)),
        ],
        compiler_params=ROOM,
        name="first",
    )(mix_angles, phase_angles, wave_parts, level_table)
    held = swap(send)
    back = pl.pallas_call(
        middle_kernel,
        out_shape=jax.ShapeDtypeStruct((64, 2, SUB, 128), F32),
        in_specs=[VMEM] * 4,
        out_specs=VMEM,
        scratch_shapes=[pltpu.VMEM((4, 16, 2, SUB, 128), F32)],
        compiler_params=ROOM,
        name="middle",
    )(aux, lanes, rows, held)
    mine = swap(back)
    out = pl.pallas_call(
        last_kernel,
        out_shape=jax.ShapeDtypeStruct((2, 4, 16, SUB, 128), F32),
        in_specs=[VMEM, VMEM],
        out_specs=HBM,
        scratch_shapes=[
            pltpu.VMEM((2, 4, 16, SUB, 128), F32),
            pltpu.VMEM((2, 4, 16, SUB, 128), F32),
            pltpu.SemaphoreType.DMA((4,)),
        ],
        compiler_params=ROOM,
        name="last",
    )(aux, mine)
    return out.reshape(2, 4, 128, 128)


def solution(mesh):
    placed = (
        P("site", ("bank", "lane"), None, None),
        P(("site", "bank", "lane"), None, None),
        P("site", None),
        P("site", None),
    )
    return jax.shard_map(
        local,
        mesh=mesh,
        in_specs=placed,
        out_specs=P("site", ("bank", "lane"), None, None),
        check_vma=False,
    )
```

```python
import jax
import jax.numpy as jnp
from jax import lax
from jax.experimental import pallas as pl
from jax.experimental.pallas import tpu as pltpu
from jax.sharding import PartitionSpec as P

SUB = 8
ORDER = [
    bank * 16 + (y + 4) % 8 * 2 + 1 - core for y in range(8) for core in range(2) for bank in (2, 0, 3, 1)
]
PLACE = [ORDER.index(k) for k in range(64)]
F32 = jnp.float32
BF16 = jnp.bfloat16

SIN = (0.9999999814442071, -0.16666657755521955, 0.008333210982283118, -0.00019834058585468524,
       2.734996203799263e-06, -2.21633008243829e-08)
COS = (0.9999999997000049, -0.4999999949621528, 0.04166665285119409, -0.0013888746708823352,
       2.4794608537121183e-05, -2.7380880775339007e-07, 1.8645524434398867e-09)


def series(z, terms):
    total = z * terms[-1] + terms[-2]
    for term in terms[-3::-1]:
        total = total * z + term
    return total


def cos_sin(x):
    z = x * x
    return series(z, COS), series(z, SIN) * x


def bit_factor(cos, sin, column, bit, row_bit):
    at = (column >> bit) & 1
    if isinstance(row_bit, bool):
        return jnp.where(at == row_bit, cos, -sin if row_bit else sin)
    return jnp.where(at == row_bit, cos, jnp.where(row_bit == 1, -sin, sin))


def low_table(cos, sin):
    row = lax.broadcasted_iota(jnp.int32, (SUB, 128), 0)
    column = lax.broadcasted_iota(jnp.int32, (SUB, 128), 1)
    tile = None
    for bit in range(3):
        factor = bit_factor(cos, sin, column, bit, (row >> bit) & 1)
        tile = factor if tile is None else tile * factor
    return tile


def seven_bits(low, high):
    column = lax.broadcasted_iota(jnp.int32, (SUB, 128), 1)
    tiles = [low_table(*low)]
    for bit in range(3, 7):
        pair = [bit_factor(*high, column, bit, at) for at in (False, True)]
        tiles = [tile * factor for factor in pair for tile in tiles]
    return jnp.concatenate(tiles, axis=0)


def halves(x):
    high = x.astype(BF16)
    return high, (x - high.astype(F32)).astype(BF16)


def dot(a, b):
    return lax.dot_general(a, b, (((1,), (0,)), ((), ())), preferred_element_type=F32)


def lane_weights(table):
    both = jnp.concatenate(halves(table), axis=1)
    return jnp.concatenate([both, both], axis=0)


def row_weights(table):
    return jnp.concatenate([jnp.concatenate([half, half], axis=1) for half in halves(table)], axis=0)


def within(parts, lanes, rows):
    count = len(parts)
    both = jnp.concatenate([jnp.concatenate(tiles, axis=0) for tiles in parts], axis=1)
    both = dot(rows, jnp.concatenate(halves(both), axis=0))
    both = both[:128] + both[128:]
    tall = jnp.concatenate([both[:, i * 128 : i * 128 + 128] for i in range(count)], axis=0)
    done = dot(jnp.concatenate(halves(tall), axis=1), lanes)
    done = done[:, :128] + done[:, 128:]
    return [[done[(j * 16 + i) * SUB : (j * 16 + i + 1) * SUB] for i in range(16)] for j in range(count)]


def mix(parts, tan):
    parts = list(parts)
    step = 1
    while step < len(parts):
        for i in range(len(parts)):
            if not i & step:
                u, v = parts[i], parts[i + step]
                parts[i], parts[i + step] = u - tan * v, v + tan * u
        step *= 2
    return parts


PHASE, SCALE, TAN2, NEXT1, NEXT2, TILES = range(6)


def trig_of(mix_ref, layer, group):
    return cos_sin(jnp.broadcast_to(mix_ref[layer : layer + 1, group : group + 1], (SUB, 128)))


def share(mix_ref, phase_ref, aux_ref, lanes_ref, rows_ref):
    scale, tans = None, {}
    for layer in range(2):
        trig = [trig_of(mix_ref, layer, group) for group in range(4)]
        for group, (cos, sin) in enumerate(trig):
            if group in (1, 2):
                tans[layer, group] = sin / cos
        back = [(cos, -sin) for cos, sin in (trig[1], trig[3])]
        cut = trig[1][0] * trig[2][0]
        cut = cut * cut
        cut = cut * cut
        scale = cut if scale is None else scale * cut
        lanes_ref[layer] = lane_weights(seven_bits(trig[0], trig[0]))
        rows_ref[layer] = row_weights(seven_bits(back[0], back[1]))
    aux_ref[PHASE] = jnp.broadcast_to(phase_ref[1:2, :], (SUB, 128))
    aux_ref[SCALE] = scale
    aux_ref[TAN2], aux_ref[NEXT1], aux_ref[NEXT2] = tans[0, 2], tans[1, 1], tans[1, 2]
    return tans[0, 1], tans[0, 2]


def first_kernel(
    mix_hbm, phase_hbm, wave_hbm, level_hbm, out_ref, aux_ref, lanes_ref, rows_ref, mix_ref, phase_ref, wave_ref, sems
):
    small = [
        pltpu.make_async_copy(mix_hbm, mix_ref, sems.at[0]),
        pltpu.make_async_copy(phase_hbm, phase_ref, sems.at[1]),
    ]
    loads = []
    for copy in small:
        copy.start()
    for b in range(4):
        pair = [
            pltpu.make_async_copy(level_hbm.at[b], out_ref.at[pl.ds(b * 16, 16), 2], sems.at[2 + 2 * b]),
            pltpu.make_async_copy(wave_hbm.at[:, b], wave_ref.at[:, b], sems.at[3 + 2 * b]),
        ]
        for copy in pair:
            copy.start()
        loads.append(pair)
    for copy in small:
        copy.wait()
    tans = share(mix_ref, phase_ref, aux_ref, lanes_ref, rows_ref)
    angle = jnp.broadcast_to(phase_ref[0:1, :], (SUB, 128))
    for b in range(4):
        for copy in loads[b]:
            copy.wait()
        re, im = [], []
        for i in range(16):
            cos, sin = cos_sin(out_ref[b * 16 + i, 2] * angle)
            u, v = wave_ref[0, b, i], wave_ref[1, b, i]
            re.append(u * cos + v * sin)
            im.append(v * cos - u * sin)
        for part, tiles in enumerate((re, im)):
            for i, tile in enumerate(mix(tiles, tans[0])):
                wave_ref[part, b, i] = tile
    for part in range(2):
        for i in range(16):
            for b, tile in enumerate(mix([wave_ref[part, b, i] for b in range(4)], tans[1])):
                out_ref[b * 16 + i, part] = tile


def middle_kernel(aux_ref, lanes_ref, rows_ref, in_ref, out_ref, work_ref):
    angle, scale = aux_ref[PHASE], aux_ref[SCALE]
    tan2, next2 = aux_ref[TAN2], aux_ref[NEXT2]
    lanes, rows = lanes_ref[0], rows_ref[0]
    for bank in range(4):
        parts = [[in_ref[PLACE[bank * 16 + i], part] for i in range(16)] for part in range(2)]
        parts = within(parts, lanes, rows)
        for part in range(2):
            for i in range(16):
                work_ref[bank, i, part] = parts[part][i]
    for i in range(16):
        re = mix([work_ref[bank, i, 0] for bank in range(4)], tan2)
        im = mix([work_ref[bank, i, 1] for bank in range(4)], tan2)
        for bank in range(4):
            cos, sin = cos_sin(in_ref[PLACE[bank * 16 + i], 2] * angle)
            cos, sin = cos * scale, sin * scale
            u, v = re[bank], im[bank]
            re[bank], im[bank] = u * cos + v * sin, v * cos - u * sin
        re, im = mix(re, next2), mix(im, next2)
        for bank in range(4):
            work_ref[bank, i, 0] = re[bank]
            work_ref[bank, i, 1] = im[bank]
    lanes, rows = lanes_ref[1], rows_ref[1]
    for bank in range(4):
        parts = within([[work_ref[bank, i, part] for i in range(16)] for part in range(2)], lanes, rows)
        for part in range(2):
            for i, tile in enumerate(parts[part]):
                out_ref[PLACE[bank * 16 + i], part] = tile


def last_kernel(aux_ref, in_ref, out_hbm, work_ref, out_ref, sems):
    next1, next2 = aux_ref[NEXT1], aux_ref[NEXT2]
    for part in range(2):
        for i in range(16):
            for b, tile in enumerate(mix([in_ref[b * 16 + i, part] for b in range(4)], next2)):
                work_ref[part, b, i] = tile
    copies = []
    for b in range(4):
        for part in range(2):
            for i, tile in enumerate(mix([work_ref[part, b, i] for i in range(16)], next1)):
                out_ref[part, b, i] = tile
        copy = pltpu.make_async_copy(out_ref.at[:, b], out_hbm.at[:, b], sems.at[b])
        copy.start()
        copies.append(copy)
    for copy in copies:
        copy.wait()


VMEM = pl.BlockSpec(memory_space=pltpu.VMEM)
HBM = pl.BlockSpec(memory_space=pltpu.HBM)
ROOM = pltpu.CompilerParams(vmem_limit_bytes=12 << 20)


def swap(values):
    return lax.all_to_all(
        values, ("bank", "lane"), split_axis=0, concat_axis=0, axis_index_groups=[ORDER], tiled=True
    )


def local(wave_parts, level_table, phase_angles, mix_angles):
    wave_parts, level_table, phase_angles, mix_angles = (
        pltpu.with_memory_space_constraint(v, pltpu.HBM)
        for v in (
            wave_parts.reshape(2, 4, 16, SUB, 128),
            level_table.reshape(4, 16, SUB, 128),
            phase_angles,
            mix_angles,
        )
    )
    send, aux, lanes, rows = pl.pallas_call(
        first_kernel,
        out_shape=(
            jax.ShapeDtypeStruct((64, 3, SUB, 128), F32),
            jax.ShapeDtypeStruct((TILES, SUB, 128), F32),
            jax.ShapeDtypeStruct((2, 256, 256), BF16),
            jax.ShapeDtypeStruct((2, 256, 256), BF16),
        ),
        in_specs=[HBM] * 4,
        out_specs=(VMEM,) * 4,
        scratch_shapes=[
            pltpu.VMEM((2, 4), F32),
            pltpu.VMEM((2, 128), F32),
            pltpu.VMEM((2, 4, 16, SUB, 128), F32),
            pltpu.SemaphoreType.DMA((10,)),
        ],
        compiler_params=ROOM,
        name="first",
    )(mix_angles, phase_angles, wave_parts, level_table)
    held = swap(send)
    back = pl.pallas_call(
        middle_kernel,
        out_shape=jax.ShapeDtypeStruct((64, 2, SUB, 128), F32),
        in_specs=[VMEM] * 4,
        out_specs=VMEM,
        scratch_shapes=[pltpu.VMEM((4, 16, 2, SUB, 128), F32)],
        compiler_params=ROOM,
        name="middle",
    )(aux, lanes, rows, held)
    mine = swap(back)
    out = pl.pallas_call(
        last_kernel,
        out_shape=jax.ShapeDtypeStruct((2, 4, 16, SUB, 128), F32),
        in_specs=[VMEM, VMEM],
        out_specs=HBM,
        scratch_shapes=[
            pltpu.VMEM((2, 4, 16, SUB, 128), F32),
            pltpu.VMEM((2, 4, 16, SUB, 128), F32),
            pltpu.SemaphoreType.DMA((4,)),
        ],
        compiler_params=ROOM,
        name="last",
    )(aux, mine)
    return out.reshape(2, 4, 128, 128)


def solution(mesh):
    placed = (
        P("site", ("bank", "lane"), None, None),
        P(("site", "bank", "lane"), None, None),
        P("site", None),
        P("site", None),
    )
    return jax.shard_map(
        local,
        mesh=mesh,
        in_specs=placed,
        out_specs=P("site", ("bank", "lane"), None, None),
        check_vma=False,
    )
```

```python
import jax
import jax.numpy as jnp
from jax import lax
from jax.experimental import pallas as pl
from jax.experimental.pallas import tpu as pltpu
from jax.sharding import PartitionSpec as P

SUB = 8
ORDER = [
    bank * 16 + (y + 4) % 8 * 2 + 1 - core for y in range(8) for core in range(2) for bank in (2, 0, 3, 1)
]
PLACE = [ORDER.index(k) for k in range(64)]
BACK = [bank * 16 + (4 + 3 * k) % 8 * 2 + core for bank in (2, 0, 3, 1) for core in (1, 0) for k in range(8)]
BACK_PLACE = [BACK.index(k) for k in range(64)]
F32 = jnp.float32
BF16 = jnp.bfloat16

SIN = (0.9999999814442071, -0.16666657755521955, 0.008333210982283118, -0.00019834058585468524,
       2.734996203799263e-06, -2.21633008243829e-08)
COS = (0.9999999997000049, -0.4999999949621528, 0.04166665285119409, -0.0013888746708823352,
       2.4794608537121183e-05, -2.7380880775339007e-07, 1.8645524434398867e-09)


def series(z, terms):
    total = z * terms[-1] + terms[-2]
    for term in terms[-3::-1]:
        total = total * z + term
    return total


def cos_sin(x):
    z = x * x
    return series(z, COS), series(z, SIN) * x


def bit_factor(cos, sin, column, bit, row_bit):
    at = (column >> bit) & 1
    if isinstance(row_bit, bool):
        return jnp.where(at == row_bit, cos, -sin if row_bit else sin)
    return jnp.where(at == row_bit, cos, jnp.where(row_bit == 1, -sin, sin))


def low_table(cos, sin):
    row = lax.broadcasted_iota(jnp.int32, (SUB, 128), 0)
    column = lax.broadcasted_iota(jnp.int32, (SUB, 128), 1)
    tile = None
    for bit in range(3):
        factor = bit_factor(cos, sin, column, bit, (row >> bit) & 1)
        tile = factor if tile is None else tile * factor
    return tile


def seven_bits(low, high):
    column = lax.broadcasted_iota(jnp.int32, (SUB, 128), 1)
    tiles = [low_table(*low)]
    for bit in range(3, 7):
        pair = [bit_factor(*high, column, bit, at) for at in (False, True)]
        tiles = [tile * factor for factor in pair for tile in tiles]
    return jnp.concatenate(tiles, axis=0)


def halves(x):
    high = x.astype(BF16)
    return high, (x - high.astype(F32)).astype(BF16)


def dot(a, b):
    return lax.dot_general(a, b, (((1,), (0,)), ((), ())), preferred_element_type=F32)


def lane_weights(table):
    both = jnp.concatenate(halves(table), axis=1)
    return jnp.concatenate([both, both], axis=0)


def row_weights(table):
    return jnp.concatenate([jnp.concatenate([half, half], axis=1) for half in halves(table)], axis=0)


def within(parts, lanes, rows):
    count = len(parts)
    both = jnp.concatenate([jnp.concatenate(tiles, axis=0) for tiles in parts], axis=1)
    both = dot(rows, jnp.concatenate(halves(both), axis=0))
    both = both[:128] + both[128:]
    tall = jnp.concatenate([both[:, i * 128 : i * 128 + 128] for i in range(count)], axis=0)
    done = dot(jnp.concatenate(halves(tall), axis=1), lanes)
    done = done[:, :128] + done[:, 128:]
    return [[done[(j * 16 + i) * SUB : (j * 16 + i + 1) * SUB] for i in range(16)] for j in range(count)]


def mix(parts, tan):
    parts = list(parts)
    step = 1
    while step < len(parts):
        for i in range(len(parts)):
            if not i & step:
                u, v = parts[i], parts[i + step]
                parts[i], parts[i + step] = u - tan * v, v + tan * u
        step *= 2
    return parts


PHASE, SCALE, TAN2, NEXT1, NEXT2, TILES = range(6)


def trig_of(mix_ref, layer, group):
    return cos_sin(jnp.broadcast_to(mix_ref[layer : layer + 1, group : group + 1], (SUB, 128)))


def share(mix_ref, phase_ref, aux_ref, lanes_ref, rows_ref):
    scale, tans = None, {}
    for layer in range(2):
        trig = [trig_of(mix_ref, layer, group) for group in range(4)]
        for group, (cos, sin) in enumerate(trig):
            if group in (1, 2):
                tans[layer, group] = sin / cos
        back = [(cos, -sin) for cos, sin in (trig[1], trig[3])]
        cut = trig[1][0] * trig[2][0]
        cut = cut * cut
        cut = cut * cut
        scale = cut if scale is None else scale * cut
        lanes_ref[layer] = lane_weights(seven_bits(trig[0], trig[0]))
        rows_ref[layer] = row_weights(seven_bits(back[0], back[1]))
    aux_ref[PHASE] = jnp.broadcast_to(phase_ref[1:2, :], (SUB, 128))
    aux_ref[SCALE] = scale
    aux_ref[TAN2], aux_ref[NEXT1], aux_ref[NEXT2] = tans[0, 2], tans[1, 1], tans[1, 2]
    return tans[0, 1], tans[0, 2]


def first_kernel(
    mix_hbm, phase_hbm, wave_hbm, level_hbm, out_ref, aux_ref, lanes_ref, rows_ref, mix_ref, phase_ref, wave_ref, sems
):
    small = [
        pltpu.make_async_copy(mix_hbm, mix_ref, sems.at[0]),
        pltpu.make_async_copy(phase_hbm, phase_ref, sems.at[1]),
    ]
    loads = []
    for copy in small:
        copy.start()
    for b in range(4):
        pair = [
            pltpu.make_async_copy(level_hbm.at[b], out_ref.at[pl.ds(b * 16, 16), 2], sems.at[2 + 2 * b]),
            pltpu.make_async_copy(wave_hbm.at[:, b], wave_ref.at[:, b], sems.at[3 + 2 * b]),
        ]
        for copy in pair:
            copy.start()
        loads.append(pair)
    for copy in small:
        copy.wait()
    tans = share(mix_ref, phase_ref, aux_ref, lanes_ref, rows_ref)
    angle = jnp.broadcast_to(phase_ref[0:1, :], (SUB, 128))
    for b in range(4):
        for copy in loads[b]:
            copy.wait()
        re, im = [], []
        for i in range(16):
            cos, sin = cos_sin(out_ref[b * 16 + i, 2] * angle)
            u, v = wave_ref[0, b, i], wave_ref[1, b, i]
            re.append(u * cos + v * sin)
            im.append(v * cos - u * sin)
        for part, tiles in enumerate((re, im)):
            for i, tile in enumerate(mix(tiles, tans[0])):
                wave_ref[part, b, i] = tile
    for part in range(2):
        for i in range(16):
            for b, tile in enumerate(mix([wave_ref[part, b, i] for b in range(4)], tans[1])):
                out_ref[b * 16 + i, part] = tile


def middle_kernel(aux_ref, lanes_ref, rows_ref, in_ref, out_ref, work_ref):
    angle, scale = aux_ref[PHASE], aux_ref[SCALE]
    tan2, next2 = aux_ref[TAN2], aux_ref[NEXT2]
    lanes, rows = lanes_ref[0], rows_ref[0]
    for bank in range(4):
        parts = [[in_ref[PLACE[bank * 16 + i], part] for i in range(16)] for part in range(2)]
        parts = within(parts, lanes, rows)
        for part in range(2):
            for i in range(16):
                work_ref[bank, i, part] = parts[part][i]
    for i in range(16):
        re = mix([work_ref[bank, i, 0] for bank in range(4)], tan2)
        im = mix([work_ref[bank, i, 1] for bank in range(4)], tan2)
        for bank in range(4):
            cos, sin = cos_sin(in_ref[PLACE[bank * 16 + i], 2] * angle)
            cos, sin = cos * scale, sin * scale
            u, v = re[bank], im[bank]
            re[bank], im[bank] = u * cos + v * sin, v * cos - u * sin
        re, im = mix(re, next2), mix(im, next2)
        for bank in range(4):
            work_ref[bank, i, 0] = re[bank]
            work_ref[bank, i, 1] = im[bank]
    lanes, rows = lanes_ref[1], rows_ref[1]
    for bank in range(4):
        parts = within([[work_ref[bank, i, part] for i in range(16)] for part in range(2)], lanes, rows)
        for part in range(2):
            for i, tile in enumerate(parts[part]):
                out_ref[BACK_PLACE[bank * 16 + i], part] = tile


def last_kernel(aux_ref, in_ref, out_hbm, work_ref, out_ref, sems):
    next1, next2 = aux_ref[NEXT1], aux_ref[NEXT2]
    for part in range(2):
        for i in range(16):
            for b, tile in enumerate(mix([in_ref[BACK_PLACE[ORDER[b * 16 + i]], part] for b in range(4)], next2)):
                work_ref[part, b, i] = tile
    copies = []
    for b in range(4):
        for part in range(2):
            for i, tile in enumerate(mix([work_ref[part, b, i] for i in range(16)], next1)):
                out_ref[part, b, i] = tile
        copy = pltpu.make_async_copy(out_ref.at[:, b], out_hbm.at[:, b], sems.at[b])
        copy.start()
        copies.append(copy)
    for copy in copies:
        copy.wait()


VMEM = pl.BlockSpec(memory_space=pltpu.VMEM)
HBM = pl.BlockSpec(memory_space=pltpu.HBM)
ROOM = pltpu.CompilerParams(vmem_limit_bytes=12 << 20)


def swap(values, order=ORDER):
    return lax.all_to_all(
        values, ("bank", "lane"), split_axis=0, concat_axis=0, axis_index_groups=[order], tiled=True
    )


def local(wave_parts, level_table, phase_angles, mix_angles):
    wave_parts, level_table, phase_angles, mix_angles = (
        pltpu.with_memory_space_constraint(v, pltpu.HBM)
        for v in (
            wave_parts.reshape(2, 4, 16, SUB, 128),
            level_table.reshape(4, 16, SUB, 128),
            phase_angles,
            mix_angles,
        )
    )
    send, aux, lanes, rows = pl.pallas_call(
        first_kernel,
        out_shape=(
            jax.ShapeDtypeStruct((64, 3, SUB, 128), F32),
            jax.ShapeDtypeStruct((TILES, SUB, 128), F32),
            jax.ShapeDtypeStruct((2, 256, 256), BF16),
            jax.ShapeDtypeStruct((2, 256, 256), BF16),
        ),
        in_specs=[HBM] * 4,
        out_specs=(VMEM,) * 4,
        scratch_shapes=[
            pltpu.VMEM((2, 4), F32),
            pltpu.VMEM((2, 128), F32),
            pltpu.VMEM((2, 4, 16, SUB, 128), F32),
            pltpu.SemaphoreType.DMA((10,)),
        ],
        compiler_params=ROOM,
        name="first",
    )(mix_angles, phase_angles, wave_parts, level_table)
    held = swap(send)
    back = pl.pallas_call(
        middle_kernel,
        out_shape=jax.ShapeDtypeStruct((64, 2, SUB, 128), F32),
        in_specs=[VMEM] * 4,
        out_specs=VMEM,
        scratch_shapes=[pltpu.VMEM((4, 16, 2, SUB, 128), F32)],
        compiler_params=ROOM,
        name="middle",
    )(aux, lanes, rows, held)
    mine = swap(back, BACK)
    out = pl.pallas_call(
        last_kernel,
        out_shape=jax.ShapeDtypeStruct((2, 4, 16, SUB, 128), F32),
        in_specs=[VMEM, VMEM],
        out_specs=HBM,
        scratch_shapes=[
            pltpu.VMEM((2, 4, 16, SUB, 128), F32),
            pltpu.VMEM((2, 4, 16, SUB, 128), F32),
            pltpu.SemaphoreType.DMA((4,)),
        ],
        compiler_params=ROOM,
        name="last",
    )(aux, mine)
    return out.reshape(2, 4, 128, 128)


def solution(mesh):
    placed = (
        P("site", ("bank", "lane"), None, None),
        P(("site", "bank", "lane"), None, None),
        P("site", None),
        P("site", None),
    )
    return jax.shard_map(
        local,
        mesh=mesh,
        in_specs=placed,
        out_specs=P("site", ("bank", "lane"), None, None),
        check_vma=False,
    )
```

```python
import jax
import jax.numpy as jnp
from jax import lax
from jax.experimental import pallas as pl
from jax.experimental.pallas import tpu as pltpu
from jax.sharding import PartitionSpec as P

SUB = 8
ORDER = [
    bank * 16 + (y + 4) % 8 * 2 + 1 - core for y in range(8) for core in range(2) for bank in (2, 0, 3, 1)
]
PLACE = [ORDER.index(k) for k in range(64)]
BACK = [bank * 16 + (4 + 3 * k) % 8 * 2 + core for bank in (2, 0, 3, 1) for core in (1, 0) for k in range(8)]
BACK_PLACE = [BACK.index(k) for k in range(64)]
F32 = jnp.float32
BF16 = jnp.bfloat16

SIN = (0.9999999814442071, -0.16666657755521955, 0.008333210982283118, -0.00019834058585468524,
       2.734996203799263e-06, -2.21633008243829e-08)
COS = (0.9999999997000049, -0.4999999949621528, 0.04166665285119409, -0.0013888746708823352,
       2.4794608537121183e-05, -2.7380880775339007e-07, 1.8645524434398867e-09)


def series(z, terms):
    total = z * terms[-1] + terms[-2]
    for term in terms[-3::-1]:
        total = total * z + term
    return total


def cos_sin(x):
    z = x * x
    return series(z, COS), series(z, SIN) * x


def bit_factor(cos, sin, column, bit, row_bit):
    at = (column >> bit) & 1
    if isinstance(row_bit, bool):
        return jnp.where(at == row_bit, cos, -sin if row_bit else sin)
    return jnp.where(at == row_bit, cos, jnp.where(row_bit == 1, -sin, sin))


def low_table(cos, sin):
    row = lax.broadcasted_iota(jnp.int32, (SUB, 128), 0)
    column = lax.broadcasted_iota(jnp.int32, (SUB, 128), 1)
    tile = None
    for bit in range(3):
        factor = bit_factor(cos, sin, column, bit, (row >> bit) & 1)
        tile = factor if tile is None else tile * factor
    return tile


def seven_bits(low, high):
    column = lax.broadcasted_iota(jnp.int32, (SUB, 128), 1)
    tiles = [low_table(*low)]
    for bit in range(3, 7):
        pair = [bit_factor(*high, column, bit, at) for at in (False, True)]
        tiles = [tile * factor for factor in pair for tile in tiles]
    return jnp.concatenate(tiles, axis=0)


def halves(x):
    high = x.astype(BF16)
    return high, (x - high.astype(F32)).astype(BF16)


def dot(a, b):
    return lax.dot_general(a, b, (((1,), (0,)), ((), ())), preferred_element_type=F32)


def lane_weights(table):
    both = jnp.concatenate(halves(table), axis=1)
    return jnp.concatenate([both, both], axis=0)


def row_weights(table):
    return jnp.concatenate([jnp.concatenate([half, half], axis=1) for half in halves(table)], axis=0)


def within(parts, lanes, rows):
    count = len(parts)
    both = jnp.concatenate([jnp.concatenate(tiles, axis=0) for tiles in parts], axis=1)
    both = dot(rows, jnp.concatenate(halves(both), axis=0))
    both = both[:128] + both[128:]
    tall = jnp.concatenate([both[:, i * 128 : i * 128 + 128] for i in range(count)], axis=0)
    done = dot(jnp.concatenate(halves(tall), axis=1), lanes)
    done = done[:, :128] + done[:, 128:]
    return [[done[(j * 16 + i) * SUB : (j * 16 + i + 1) * SUB] for i in range(16)] for j in range(count)]


def mix(parts, tan):
    parts = list(parts)
    step = 1
    while step < len(parts):
        for i in range(len(parts)):
            if not i & step:
                u, v = parts[i], parts[i + step]
                parts[i], parts[i + step] = u - tan * v, v + tan * u
        step *= 2
    return parts


PHASE, SCALE, TAN2, NEXT1, NEXT2, TILES = range(6)


def trig_of(mix_ref, layer, group):
    return cos_sin(jnp.broadcast_to(mix_ref[layer : layer + 1, group : group + 1], (SUB, 128)))


def share(mix_ref, phase_ref, aux_ref, lanes_ref, rows_ref):
    scale, tans = None, {}
    for layer in range(2):
        trig = [trig_of(mix_ref, layer, group) for group in range(4)]
        for group, (cos, sin) in enumerate(trig):
            if group in (1, 2):
                tans[layer, group] = sin / cos
        back = [(cos, -sin) for cos, sin in (trig[1], trig[3])]
        cut = trig[1][0] * trig[2][0]
        cut = cut * cut
        cut = cut * cut
        scale = cut if scale is None else scale * cut
        lanes_ref[layer] = lane_weights(seven_bits(trig[0], trig[0]))
        rows_ref[layer] = row_weights(seven_bits(back[0], back[1]))
    aux_ref[PHASE] = jnp.broadcast_to(phase_ref[1:2, :], (SUB, 128))
    aux_ref[SCALE] = scale
    aux_ref[TAN2], aux_ref[NEXT1], aux_ref[NEXT2] = tans[0, 2], tans[1, 1], tans[1, 2]
    return tans[0, 1], tans[0, 2]


def first_kernel(
    mix_hbm, phase_hbm, wave_hbm, level_hbm, out_ref, aux_ref, lanes_ref, rows_ref, mix_ref, phase_ref, wave_ref, sems
):
    small = [
        pltpu.make_async_copy(mix_hbm, mix_ref, sems.at[0]),
        pltpu.make_async_copy(phase_hbm, phase_ref, sems.at[1]),
    ]
    loads = []
    for copy in small:
        copy.start()
    for b in range(4):
        pair = [
            pltpu.make_async_copy(level_hbm.at[b], out_ref.at[pl.ds(b * 16, 16), 2], sems.at[2 + 2 * b]),
            pltpu.make_async_copy(wave_hbm.at[:, b], wave_ref.at[:, b], sems.at[3 + 2 * b]),
        ]
        for copy in pair:
            copy.start()
        loads.append(pair)
    for copy in small:
        copy.wait()
    tans = share(mix_ref, phase_ref, aux_ref, lanes_ref, rows_ref)
    angle = jnp.broadcast_to(phase_ref[0:1, :], (SUB, 128))
    for b in range(4):
        for copy in loads[b]:
            copy.wait()
        re, im = [], []
        for i in range(16):
            cos, sin = cos_sin(out_ref[b * 16 + i, 2] * angle)
            u, v = wave_ref[0, b, i], wave_ref[1, b, i]
            re.append(u * cos + v * sin)
            im.append(v * cos - u * sin)
        for part, tiles in enumerate((re, im)):
            for i, tile in enumerate(mix(tiles, tans[0])):
                wave_ref[part, b, i] = tile
    for part in range(2):
        for i in range(16):
            for b, tile in enumerate(mix([wave_ref[part, b, i] for b in range(4)], tans[1])):
                out_ref[b * 16 + i, part] = tile


def middle_kernel(aux_ref, lanes_ref, rows_ref, in_ref, out_ref, work_ref):
    angle, scale = aux_ref[PHASE], aux_ref[SCALE]
    tan2, next2 = aux_ref[TAN2], aux_ref[NEXT2]
    lanes, rows = lanes_ref[0], rows_ref[0]
    for bank in range(4):
        parts = [[in_ref[PLACE[bank * 16 + i], part] for i in range(16)] for part in range(2)]
        parts = within(parts, lanes, rows)
        for part in range(2):
            for i in range(16):
                work_ref[bank, i, part] = parts[part][i]
    for i in range(16):
        re = mix([work_ref[bank, i, 0] for bank in range(4)], tan2)
        im = mix([work_ref[bank, i, 1] for bank in range(4)], tan2)
        for bank in range(4):
            cos, sin = cos_sin(in_ref[PLACE[bank * 16 + i], 2] * angle)
            cos, sin = cos * scale, sin * scale
            u, v = re[bank], im[bank]
            re[bank], im[bank] = u * cos + v * sin, v * cos - u * sin
        re, im = mix(re, next2), mix(im, next2)
        for bank in range(4):
            work_ref[bank, i, 0] = re[bank]
            work_ref[bank, i, 1] = im[bank]
    lanes, rows = lanes_ref[1], rows_ref[1]
    for bank in range(4):
        parts = within([[work_ref[bank, i, part] for i in range(16)] for part in range(2)], lanes, rows)
        for part in range(2):
            for i, tile in enumerate(parts[part]):
                out_ref[BACK_PLACE[bank * 16 + i], part] = tile


def last_kernel(aux_ref, in_ref, out_hbm, work_ref, out_ref, sems):
    next1, next2 = aux_ref[NEXT1], aux_ref[NEXT2]
    for part in range(2):
        for i in range(16):
            for b, tile in enumerate(mix([in_ref[BACK_PLACE[ORDER[b * 16 + i]], part] for b in range(4)], next2)):
                work_ref[part, b, i] = tile
    copies = []
    for b in range(4):
        for part in range(2):
            for i, tile in enumerate(mix([work_ref[part, b, i] for i in range(16)], next1)):
                out_ref[part, b, i] = tile
            copy = pltpu.make_async_copy(out_ref.at[part, b], out_hbm.at[part, b], sems.at[b * 2 + part])
            copy.start()
            copies.append(copy)
    for copy in copies:
        copy.wait()


VMEM = pl.BlockSpec(memory_space=pltpu.VMEM)
HBM = pl.BlockSpec(memory_space=pltpu.HBM)
ROOM = pltpu.CompilerParams(vmem_limit_bytes=12 << 20)


def swap(values, order=ORDER):
    return lax.all_to_all(
        values, ("bank", "lane"), split_axis=0, concat_axis=0, axis_index_groups=[order], tiled=True
    )


def local(wave_parts, level_table, phase_angles, mix_angles):
    wave_parts, level_table, phase_angles, mix_angles = (
        pltpu.with_memory_space_constraint(v, pltpu.HBM)
        for v in (
            wave_parts.reshape(2, 4, 16, SUB, 128),
            level_table.reshape(4, 16, SUB, 128),
            phase_angles,
            mix_angles,
        )
    )
    send, aux, lanes, rows = pl.pallas_call(
        first_kernel,
        out_shape=(
            jax.ShapeDtypeStruct((64, 3, SUB, 128), F32),
            jax.ShapeDtypeStruct((TILES, SUB, 128), F32),
            jax.ShapeDtypeStruct((2, 256, 256), BF16),
            jax.ShapeDtypeStruct((2, 256, 256), BF16),
        ),
        in_specs=[HBM] * 4,
        out_specs=(VMEM,) * 4,
        scratch_shapes=[
            pltpu.VMEM((2, 4), F32),
            pltpu.VMEM((2, 128), F32),
            pltpu.VMEM((2, 4, 16, SUB, 128), F32),
            pltpu.SemaphoreType.DMA((10,)),
        ],
        compiler_params=ROOM,
        name="first",
    )(mix_angles, phase_angles, wave_parts, level_table)
    held = swap(send)
    back = pl.pallas_call(
        middle_kernel,
        out_shape=jax.ShapeDtypeStruct((64, 2, SUB, 128), F32),
        in_specs=[VMEM] * 4,
        out_specs=VMEM,
        scratch_shapes=[pltpu.VMEM((4, 16, 2, SUB, 128), F32)],
        compiler_params=ROOM,
        name="middle",
    )(aux, lanes, rows, held)
    mine = swap(back, BACK)
    out = pl.pallas_call(
        last_kernel,
        out_shape=jax.ShapeDtypeStruct((2, 4, 16, SUB, 128), F32),
        in_specs=[VMEM, VMEM],
        out_specs=HBM,
        scratch_shapes=[
            pltpu.VMEM((2, 4, 16, SUB, 128), F32),
            pltpu.VMEM((2, 4, 16, SUB, 128), F32),
            pltpu.SemaphoreType.DMA((8,)),
        ],
        compiler_params=ROOM,
        name="last",
    )(aux, mine)
    return out.reshape(2, 4, 128, 128)


def solution(mesh):
    placed = (
        P("site", ("bank", "lane"), None, None),
        P(("site", "bank", "lane"), None, None),
        P("site", None),
        P("site", None),
    )
    return jax.shard_map(
        local,
        mesh=mesh,
        in_specs=placed,
        out_specs=P("site", ("bank", "lane"), None, None),
        check_vma=False,
    )
```
